32 devices in a mesh: expert: 4 (over x, core), shard: 8 (over z, y).
Axes of the slice: x: 2, y: 2, z: 4, core: 2. Of those that a mesh axis runs over, the one named last changes fastest.
Arguments:
- master_gate: float32 [64, 2048, 1024], P('expert', 'shard'), may hold values from -0.1875 to 0.1875
- master_up: float32 [64, 2048, 1024], P('expert', 'shard'), may hold values from -0.1875 to 0.1875
- master_down: float32 [64, 1024, 2048], P('expert', None, 'shard'), may hold values from -0.25 to 0.25
- router_weight: float32 [2048, 64], P('shard', 'expert'), may hold values from -0.125 to 0.125
- router_gain: float32 [2048], P('shard'), may hold values from 0.25 to 1.75
Outputs:
- final_gate: bfloat16 [64, 2048, 1024], P('expert', None, 'shard')
- final_up: bfloat16 [64, 2048, 1024], P('expert', None, 'shard')
- final_down: bfloat16 [64, 1024, 2048], P('expert', 'shard')
- scale_gate: float32 [64, 1024], P('expert', 'shard')
- scale_up: float32 [64, 1024], P('expert', 'shard')
- scale_down: float32 [64, 1024], P('expert', 'shard')
- serve_router: bfloat16 [2048, 64], replicated
The draws below stay inside these ranges and needn't reach their ends.
All inputs are finite; a program needn't handle non-finite values.
Results may differ from the reference program's by a relative error of at most 0.001.
Values may be sent and summed in bfloat16 or wider, within the bound.
A program may use at most 192 MiB of HBM per device.

```python
import jax
import jax.numpy as jnp
from jax import lax

EXPERTS = 64
D_MODEL = 2048
D_EXPERT = 1024


def with_spikes(entries, rng, source, target, shards_of, factor):
    def block_of(axis_at):
        return (jnp.arange(entries.shape[axis_at]) // (entries.shape[axis_at] // shards_of)).reshape((-1,) + (1,) * (entries.ndim - 1 - axis_at))

    first = jax.random.permutation(rng, shards_of)[block_of(target)]
    far = (block_of(target) + shards_of // 2) % shards_of
    return jnp.where((block_of(source) == first) | (block_of(source) == far), factor * entries, entries)


def levels(stream_key, dims, split, smallest, high):
    factor_of = 1.0
    for position, parts in split:
        steps = jax.random.uniform(jax.random.fold_in(jax.random.fold_in(stream_key, 6), position), (parts,), jnp.float32, smallest / len(split), high / len(split))
        factor_of = factor_of * jnp.repeat(jnp.exp(steps), dims[position] // parts).reshape((-1,) + (1,) * (len(dims) - 1 - position))
    return factor_of


def centred(stream_key, extent, width, bound, split=(), held_as=jnp.bfloat16):
    entries = width * jax.random.normal(stream_key, extent, jnp.float32)
    if split:
        entries = entries * levels(stream_key, extent, split, -0.22, 0.18)
    return jnp.clip(entries, -bound, bound).astype(held_as)


def bell_draw_with(rng, dims, spread, reach, pieces, heavy, dtype=jnp.bfloat16):
    values = spread * jax.random.normal(rng, dims, jnp.float32)
    if pieces:
        values = values * levels(rng, dims, pieces, -0.22, 0.18)
    return jnp.clip(with_spikes(values, jax.random.fold_in(rng, 3), *heavy), -reach, reach).astype(dtype)


def setup_inputs(seed: int = 0) -> dict:
    streams_of = jax.random.split(jax.random.key(seed), 6)
    return {
        "master_gate": bell_draw_with(streams_of[0], (EXPERTS, D_MODEL, D_EXPERT), D_MODEL ** -0.5, 0.1875, ((0, 4), (1, 8)), (1, 2, 8, 2.0), jnp.float32),
        "master_up": bell_draw_with(streams_of[1], (EXPERTS, D_MODEL, D_EXPERT), D_MODEL ** -0.5, 0.1875, ((0, 4), (1, 8)), (1, 2, 8, 2.0), jnp.float32),
        "master_down": bell_draw_with(streams_of[2], (EXPERTS, D_EXPERT, D_MODEL), D_EXPERT ** -0.5, 0.25, ((0, 4), (2, 8)), (2, 1, 8, 2.0), jnp.float32),
        "router_weight": centred(streams_of[3], (D_MODEL, EXPERTS), D_MODEL ** -0.5, 0.125, ((0, 8), (1, 4)), jnp.float32),
        "router_gain": jnp.clip(1.0 + 0.15 * jax.random.normal(streams_of[4], (D_MODEL,), jnp.float32), 0.25, 1.75),
    }


def reference(master_gate, master_up, master_down, router_weight, router_gain):
    scale_gate = jnp.sqrt(lax.optimization_barrier(jnp.sum(master_gate * master_gate, axis=1)))
    final_gate = (master_gate / jnp.expand_dims(scale_gate, 1)).astype(jnp.bfloat16)
    scale_up = jnp.sqrt(lax.optimization_barrier(jnp.sum(master_up * master_up, axis=1)))
    final_up = (master_up / jnp.expand_dims(scale_up, 1)).astype(jnp.bfloat16)
    scale_down = jnp.sqrt(lax.optimization_barrier(jnp.sum(master_down * master_down, axis=2)))
    final_down = (master_down / jnp.expand_dims(scale_down, 2)).astype(jnp.bfloat16)
    serve_router = (router_weight * router_gain[:, None]).astype(jnp.bfloat16)
    return (final_gate, final_up, final_down, scale_gate, scale_up, scale_down, serve_router)
```

```python
import functools

import jax
import jax.numpy as jnp
from jax import lax
from jax.experimental import pallas as pl
from jax.experimental.pallas import tpu as pltpu
from jax.sharding import PartitionSpec as P

MESH = pl.DeviceIdType.MESH
SLOTS = 4


def exchange(
    n, groups, gate, up, down, weight, gain,
    out_gate, out_up, out_down, scale_gate, scale_up, scale_down, out_router,
    in_gate, in_up, in_down, send_gate, send_up, send_down,
    part, arrived, owned, inverse, narrow_router,
    load_sem, part_send, part_recv, inv_send, inv_recv,
    big_send, big_recv, own_sem, router_sem,
):
    experts, rows, width = gate.shape
    cols = width // n
    me = lax.axis_index("shard")
    grp = lax.axis_index("expert")
    order = sorted(range(1, n), key=lambda k: (abs(2 * k - n), k))
    lanes = min(128, down.shape[2])

    def peer(k):
        return lax.rem(me + k, n)

    def load(t):
        slot = lax.rem(t, SLOTS)
        return [
            pltpu.make_async_copy(src.at[t], dst.at[slot], load_sem.at[slot, i])
            for i, (src, dst) in enumerate(((gate, in_gate), (up, in_up), (down, in_down)))
        ]

    for copy in load(0):
        copy.start()

    barrier = pltpu.get_barrier_semaphore()
    for k in range(1, n):
        pl.semaphore_signal(barrier, inc=1, device_id={"shard": peer(k)}, device_id_type=MESH)
    for k in range(1, groups):
        pl.semaphore_signal(
            barrier, inc=1, device_id={"expert": lax.rem(grp + k, groups)}, device_id_type=MESH
        )

    w = weight[...]
    experts_here, depth = w.shape
    narrow_router[...] = (w * gain[...]).astype(jnp.bfloat16)
    router_rows = pl.ds(pl.multiple_of(grp * experts_here, experts_here), experts_here)
    router_cols = pl.ds(pl.multiple_of(me * depth, depth), depth)

    pl.semaphore_wait(barrier, n - 1 + groups - 1)

    def router_first(k):
        return pltpu.make_async_remote_copy(
            src_ref=narrow_router,
            dst_ref=out_router.at[router_rows, router_cols],
            send_sem=router_sem.at[0],
            recv_sem=router_sem.at[1],
            device_id={"shard": peer(k)},
            device_id_type=MESH,
        )

    router_own = pltpu.make_async_copy(
        narrow_router, out_router.at[router_rows, router_cols], router_sem.at[2]
    )

    def router_second(k):
        return pltpu.make_async_remote_copy(
            src_ref=out_router.at[router_rows, :],
            dst_ref=out_router.at[router_rows, :],
            send_sem=router_sem.at[3],
            recv_sem=router_sem.at[4],
            device_id={"expert": lax.rem(grp + k, groups)},
            device_id_type=MESH,
        )

    def sums(t):
        @pl.when(t + 1 < experts)
        def _():
            for copy in load(t + 1):
                copy.start()

        for copy in load(t):
            copy.wait()
        slot = lax.rem(t, SLOTS)
        for i, ref in enumerate((in_gate, in_up)):
            for d in range(n):
                x = ref[slot, :, d * cols:(d + 1) * cols]
                part[t, d, i] = jnp.sum(x * x, axis=0, keepdims=True)
        for d in range(n):
            x = in_down[slot, d * cols:(d + 1) * cols, :]
            x = x * x
            folded = x[:, :lanes]
            for c in range(lanes, x.shape[1], lanes):
                folded = folded + x[:, c:c + lanes]
            part[t, d, 2] = jnp.sum(folded.T, axis=0, keepdims=True)
        for k in order:
            pltpu.make_async_remote_copy(
                src_ref=part.at[t, peer(k)],
                dst_ref=arrived.at[t, k - 1],
                send_sem=part_send,
                recv_sem=part_recv.at[t],
                device_id={"shard": peer(k)},
                device_id_type=MESH,
            ).start()

    def reduce(t):
        pltpu.make_async_copy(arrived.at[t], arrived.at[t], part_recv.at[t]).wait()
        for i, out in enumerate((scale_gate, scale_up, scale_down)):
            total = part[t, me, i]
            for k in range(n - 1):
                total = total + arrived[t, k, i]
            scale = jnp.sqrt(total)
            out[pl.ds(t, 1), :] = scale
            owned[t, i] = 1.0 / scale
            inverse[t, me, i] = 1.0 / scale
        for k in order:
            pltpu.make_async_remote_copy(
                src_ref=owned.at[t],
                dst_ref=inverse.at[t, me],
                send_sem=inv_send,
                recv_sem=inv_recv.at[t],
                device_id={"shard": peer(k)},
                device_id_type=MESH,
            ).start()

    row_at = pl.ds(pl.multiple_of(me * rows, rows), rows)
    col_at = pl.ds(pl.multiple_of(me * down.shape[2], down.shape[2]), down.shape[2])

    def places(t):
        return (
            (send_gate, out_gate.at[t, row_at, :]),
            (send_up, out_up.at[t, row_at, :]),
            (send_down, out_down.at[t, :, col_at]),
        )

    def finish(t):
        pltpu.make_async_copy(
            inverse.at[t, pl.ds(0, n - 1)], inverse.at[t, pl.ds(0, n - 1)], inv_recv.at[t]
        ).wait()
        slot = lax.rem(t, SLOTS)
        for i, (ref, send) in enumerate(((in_gate, send_gate), (in_up, send_up))):
            for d in range(n):
                x = ref[slot, :, d * cols:(d + 1) * cols]
                send[t, d] = (x * inverse[t, d, i]).astype(jnp.bfloat16)
        for d in range(n):
            across = jnp.broadcast_to(inverse[t, d, 2], (lanes, cols)).T
            for c in range(0, down.shape[2], lanes):
                x = in_down[slot, d * cols:(d + 1) * cols, c:c + lanes]
                send_down[t, d, :, c:c + lanes] = (x * across).astype(jnp.bfloat16)
        for i, (send, place) in enumerate(places(t)):
            for k in order:
                pltpu.make_async_remote_copy(
                    src_ref=send.at[t, peer(k)],
                    dst_ref=place,
                    send_sem=big_send.at[i],
                    recv_sem=big_recv.at[i],
                    device_id={"shard": peer(k)},
                    device_id_type=MESH,
                ).start()
            pltpu.make_async_copy(send.at[t, me], place, own_sem.at[i]).start()

    def step(t, carry):
        @pl.when(t < experts)
        def _():
            sums(t)

        @pl.when(t == 0)
        def _():
            router_own.start()
            for k in order:
                router_first(k).start()

        @pl.when((t >= 1) & (t <= experts))
        def _():
            reduce(t - 1)

        @pl.when(t >= 2)
        def _():
            finish(t - 2)

        return carry

    lax.fori_loop(0, experts + 2, step, 0)

    router_own.wait()
    gathered = out_router.at[router_rows, pl.ds(0, (n - 1) * depth)]
    pltpu.make_async_copy(gathered, gathered, router_sem.at[1]).wait()
    for k in range(1, groups):
        router_second(k).start()

    others = pl.ds(0, n - 1)
    for i, send in enumerate((send_gate, send_up, send_down)):
        blocks = send.at[:, others]
        pltpu.make_async_copy(blocks, blocks, big_recv.at[i]).wait()
        pltpu.make_async_copy(blocks, blocks, big_send.at[i]).wait()
        mine = send.at[:, 0]
        pltpu.make_async_copy(mine, mine, own_sem.at[i]).wait()
    pltpu.make_async_copy(arrived, arrived, part_send).wait()
    pltpu.make_async_copy(inverse.at[:, others], inverse.at[:, others], inv_send).wait()
    pltpu.make_async_copy(gathered, gathered, router_sem.at[0]).wait()
    handed = out_router.at[pl.ds(0, (groups - 1) * experts_here), :]
    pltpu.make_async_copy(handed, handed, router_sem.at[3]).wait()
    pltpu.make_async_copy(handed, handed, router_sem.at[4]).wait()


def by_collectives(master_gate, master_up, master_down, router_weight, router_gain):
    total_gate, total_up, total_down = lax.psum(
        (
            jnp.sum(master_gate * master_gate, axis=1),
            jnp.sum(master_up * master_up, axis=1),
            jnp.sum(master_down * master_down, axis=2),
        ),
        "shard",
    )
    scale_gate = jnp.sqrt(total_gate)
    scale_up = jnp.sqrt(total_up)
    scale_down = jnp.sqrt(total_down)
    narrow_gate, narrow_up, narrow_down = (
        (master_gate / jnp.expand_dims(scale_gate, 1)).astype(jnp.bfloat16),
        (master_up / jnp.expand_dims(scale_up, 1)).astype(jnp.bfloat16),
        (master_down / jnp.expand_dims(scale_down, 2)).astype(jnp.bfloat16),
    )
    final_gate, final_up = (
        lax.all_to_all(narrow_gate, "shard", split_axis=2, concat_axis=1, tiled=True),
        lax.all_to_all(narrow_up, "shard", split_axis=2, concat_axis=1, tiled=True),
    )
    final_down = lax.all_to_all(narrow_down, "shard", split_axis=1, concat_axis=2, tiled=True)
    scale_gate = lax.dynamic_slice_in_dim(
        scale_gate, lax.axis_index("shard") * final_gate.shape[2], final_gate.shape[2], axis=1
    )
    scale_up = lax.dynamic_slice_in_dim(
        scale_up, lax.axis_index("shard") * final_up.shape[2], final_up.shape[2], axis=1
    )
    scale_down = lax.dynamic_slice_in_dim(
        scale_down, lax.axis_index("shard") * final_down.shape[1], final_down.shape[1], axis=1
    )
    part_router = (router_weight * router_gain[:, None]).astype(jnp.bfloat16)
    row_router = lax.all_gather(part_router, "shard", axis=0, tiled=True)
    serve_router = lax.all_gather(row_router, "expert", axis=1, tiled=True)
    return (final_gate, final_up, final_down, scale_gate, scale_up, scale_down, serve_router)


def on_device(n, groups, gate, up, down, router_weight, router_gain):
    experts, rows, width = gate.shape
    cols = width // n
    inner = down.shape[2]
    depth, experts_here = router_weight.shape
    if cols % 128 or inner % 128 or depth % 128:
        return by_collectives(gate, up, down, router_weight, router_gain)
    narrow, wide = jnp.bfloat16, jnp.float32
    dma = pltpu.SemaphoreType.DMA
    any_space = pl.BlockSpec(memory_space=pl.ANY)
    vmem = pl.BlockSpec(memory_space=pltpu.VMEM)
    outs = pl.pallas_call(
        functools.partial(exchange, n, groups),
        out_shape=(
            jax.ShapeDtypeStruct((experts, rows * n, cols), narrow),
            jax.ShapeDtypeStruct((experts, rows * n, cols), narrow),
            jax.ShapeDtypeStruct((experts, cols, inner * n), narrow),
            jax.ShapeDtypeStruct((experts, cols), wide),
            jax.ShapeDtypeStruct((experts, cols), wide),
            jax.ShapeDtypeStruct((experts, cols), wide),
            jax.ShapeDtypeStruct((experts_here * groups, depth * n), narrow),
        ),
        in_specs=[any_space] * 3 + [vmem] * 2,
        out_specs=(any_space,) * 3 + (vmem,) * 3 + (any_space,),
        scratch_shapes=[
            pltpu.VMEM((SLOTS, rows, width), wide),
            pltpu.VMEM((SLOTS, rows, width), wide),
            pltpu.VMEM((SLOTS, width, inner), wide),
            pltpu.VMEM((experts, n, rows, cols), narrow),
            pltpu.VMEM((experts, n, rows, cols), narrow),
            pltpu.VMEM((experts, n, cols, inner), narrow),
            pltpu.VMEM((experts, n, 3, 1, cols), wide),
            pltpu.VMEM((experts, n - 1, 3, 1, cols), wide),
            pltpu.VMEM((experts, 3, 1, cols), wide),
            pltpu.VMEM((experts, n, 3, 1, cols), wide),
            pltpu.VMEM((experts_here, depth), narrow),
            dma((SLOTS, 3)),
            dma,
            dma((experts,)),
            dma,
            dma((experts,)),
            dma((3,)),
            dma((3,)),
            dma((3,)),
            dma((5,)),
        ],
        compiler_params=pltpu.CompilerParams(
            collective_id=0, has_side_effects=True, vmem_limit_bytes=60 * 2**20
        ),
    )(gate, up, down, router_weight.T, router_gain[None, :])
    return outs[:6] + (outs[6].T,)


def solution(mesh):
    placed = (
        P("expert", "shard", None),
        P("expert", "shard", None),
        P("expert", None, "shard"),
        P("shard", "expert"),
        P("shard"),
    )
    return jax.shard_map(
        functools.partial(on_device, mesh.shape["shard"], mesh.shape["expert"]),
        mesh=mesh,
        in_specs=placed,
        out_specs=(
            P("expert", None, "shard"),
            P("expert", None, "shard"),
            P("expert", "shard", None),
            P("expert", "shard"),
            P("expert", "shard"),
            P("expert", "shard"),
            P(),
        ),
        check_vma=False,
    )
```

```python
import functools

import jax
import jax.numpy as jnp
from jax import lax
from jax.experimental import pallas as pl
from jax.experimental.pallas import tpu as pltpu
from jax.sharding import PartitionSpec as P

MESH = pl.DeviceIdType.MESH
SLOTS = 4


def exchange(
    n, groups, gate, up, down, weight, gain,
    out_gate, out_up, out_down, scale_gate, scale_up, scale_down, out_router, later,
    in_gate, in_up, in_down, send_gate, send_up, send_down,
    part, arrived, owned, inverse, narrow_router,
    load_sem, part_send, part_recv, inv_send, inv_recv,
    big_send, big_recv, own_sem, router_sem,
):
    experts, rows, width = gate.shape
    early = out_down.shape[0]
    cols = width // n
    me = lax.axis_index("shard")
    grp = lax.axis_index("expert")
    order = sorted(range(1, n), key=lambda k: (abs(2 * k - n), k))
    lanes = min(128, down.shape[2])

    def peer(k):
        return lax.rem(me + k, n)

    def load(t):
        slot = lax.rem(t, SLOTS)
        return [
            pltpu.make_async_copy(src.at[t], dst.at[slot], load_sem.at[slot, i])
            for i, (src, dst) in enumerate(((gate, in_gate), (up, in_up), (down, in_down)))
        ]

    for copy in load(0):
        copy.start()

    barrier = pltpu.get_barrier_semaphore()
    for k in range(1, n):
        pl.semaphore_signal(barrier, inc=1, device_id={"shard": peer(k)}, device_id_type=MESH)
    for k in range(1, groups):
        pl.semaphore_signal(
            barrier, inc=1, device_id={"expert": lax.rem(grp + k, groups)}, device_id_type=MESH
        )

    w = weight[...]
    experts_here, depth = w.shape
    narrow_router[...] = (w * gain[...]).astype(jnp.bfloat16)
    router_rows = pl.ds(pl.multiple_of(grp * experts_here, experts_here), experts_here)
    router_cols = pl.ds(pl.multiple_of(me * depth, depth), depth)

    pl.semaphore_wait(barrier, n - 1 + groups - 1)

    def router_first(k):
        return pltpu.make_async_remote_copy(
            src_ref=narrow_router,
            dst_ref=out_router.at[router_rows, router_cols],
            send_sem=router_sem.at[0],
            recv_sem=router_sem.at[1],
            device_id={"shard": peer(k)},
            device_id_type=MESH,
        )

    router_own = pltpu.make_async_copy(
        narrow_router, out_router.at[router_rows, router_cols], router_sem.at[2]
    )

    def router_second(k):
        return pltpu.make_async_remote_copy(
            src_ref=out_router.at[router_rows, :],
            dst_ref=out_router.at[router_rows, :],
            send_sem=router_sem.at[3],
            recv_sem=router_sem.at[4],
            device_id={"expert": lax.rem(grp + k, groups)},
            device_id_type=MESH,
        )

    def sums(t):
        @pl.when(t + 1 < experts)
        def _():
            for copy in load(t + 1):
                copy.start()

        for copy in load(t):
            copy.wait()
        slot = lax.rem(t, SLOTS)
        for i, ref in enumerate((in_gate, in_up)):
            for d in range(n):
                x = ref[slot, :, d * cols:(d + 1) * cols]
                part[t, d, i] = jnp.sum(x * x, axis=0, keepdims=True)
        for d in range(n):
            x = in_down[slot, d * cols:(d + 1) * cols, :]
            x = x * x
            folded = x[:, :lanes]
            for c in range(lanes, x.shape[1], lanes):
                folded = folded + x[:, c:c + lanes]
            part[t, d, 2] = jnp.sum(folded.T, axis=0, keepdims=True)
        for k in order:
            pltpu.make_async_remote_copy(
                src_ref=part.at[t, peer(k)],
                dst_ref=arrived.at[t, k - 1],
                send_sem=part_send,
                recv_sem=part_recv.at[t],
                device_id={"shard": peer(k)},
                device_id_type=MESH,
            ).start()

    def reduce(t):
        pltpu.make_async_copy(arrived.at[t], arrived.at[t], part_recv.at[t]).wait()
        for i, out in enumerate((scale_gate, scale_up, scale_down)):
            total = part[t, me, i]
            for k in range(n - 1):
                total = total + arrived[t, k, i]
            scale = jnp.sqrt(total)
            out[pl.ds(t, 1), :] = scale
            owned[t, i] = 1.0 / scale
            inverse[t, me, i] = 1.0 / scale
        for k in order:
            pltpu.make_async_remote_copy(
                src_ref=owned.at[t],
                dst_ref=inverse.at[t, me],
                send_sem=inv_send,
                recv_sem=inv_recv.at[t],
                device_id={"shard": peer(k)},
                device_id_type=MESH,
            ).start()

    row_at = pl.ds(pl.multiple_of(me * rows, rows), rows)
    col_at = pl.ds(pl.multiple_of(me * down.shape[2], down.shape[2]), down.shape[2])

    def spread(t, i, send, place):
        for k in order:
            pltpu.make_async_remote_copy(
                src_ref=send.at[t, peer(k)],
                dst_ref=place,
                send_sem=big_send.at[i],
                recv_sem=big_recv.at[i],
                device_id={"shard": peer(k)},
                device_id_type=MESH,
            ).start()
        pltpu.make_async_copy(send.at[t, me], place, own_sem.at[i]).start()

    def finish(t):
        pltpu.make_async_copy(
            inverse.at[t, pl.ds(0, n - 1)], inverse.at[t, pl.ds(0, n - 1)], inv_recv.at[t]
        ).wait()
        slot = lax.rem(t, SLOTS)
        for i, (ref, send, out) in enumerate(
            ((in_gate, send_gate, out_gate), (in_up, send_up, out_up))
        ):
            for d in range(n):
                x = ref[slot, :, d * cols:(d + 1) * cols]
                send[t, d] = (x * inverse[t, d, i]).astype(jnp.bfloat16)
            spread(t, i, send, out.at[t, row_at, :])
        for d in range(n):
            across = jnp.broadcast_to(inverse[t, d, 2], (lanes, cols)).T
            for c in range(0, down.shape[2], lanes):
                x = in_down[slot, d * cols:(d + 1) * cols, c:c + lanes]
                send_down[t, d, :, c:c + lanes] = (x * across).astype(jnp.bfloat16)

        @pl.when(t < early)
        def _():
            spread(t, 2, send_down, out_down.at[t, :, col_at])

        @pl.when(t >= early)
        def _():
            pltpu.make_async_copy(send_down.at[t], later.at[:, t - early], own_sem.at[3]).start()

    def step(t, carry):
        @pl.when(t < experts)
        def _():
            sums(t)

        @pl.when(t == 0)
        def _():
            router_own.start()
            for k in order:
                router_first(k).start()

        @pl.when((t >= 1) & (t <= experts))
        def _():
            reduce(t - 1)

        @pl.when(t >= 2)
        def _():
            finish(t - 2)

        return carry

    lax.fori_loop(0, experts + 2, step, 0)

    router_own.wait()
    gathered = out_router.at[router_rows, pl.ds(0, (n - 1) * depth)]
    pltpu.make_async_copy(gathered, gathered, router_sem.at[1]).wait()
    for k in range(1, groups):
        router_second(k).start()

    others = pl.ds(0, n - 1)
    pltpu.make_async_copy(later, later, own_sem.at[3]).wait()
    for i, (send, sent) in enumerate(
        ((send_gate, experts), (send_up, experts), (send_down, early))
    ):
        blocks = send.at[pl.ds(0, sent), others]
        pltpu.make_async_copy(blocks, blocks, big_recv.at[i]).wait()
        pltpu.make_async_copy(blocks, blocks, big_send.at[i]).wait()
        mine = send.at[pl.ds(0, sent), 0]
        pltpu.make_async_copy(mine, mine, own_sem.at[i]).wait()
    pltpu.make_async_copy(arrived, arrived, part_send).wait()
    pltpu.make_async_copy(inverse.at[:, others], inverse.at[:, others], inv_send).wait()
    pltpu.make_async_copy(gathered, gathered, router_sem.at[0]).wait()
    handed = out_router.at[pl.ds(0, (groups - 1) * experts_here), :]
    pltpu.make_async_copy(handed, handed, router_sem.at[3]).wait()
    pltpu.make_async_copy(handed, handed, router_sem.at[4]).wait()


def by_collectives(master_gate, master_up, master_down, router_weight, router_gain):
    total_gate, total_up, total_down = lax.psum(
        (
            jnp.sum(master_gate * master_gate, axis=1),
            jnp.sum(master_up * master_up, axis=1),
            jnp.sum(master_down * master_down, axis=2),
        ),
        "shard",
    )
    scale_gate = jnp.sqrt(total_gate)
    scale_up = jnp.sqrt(total_up)
    scale_down = jnp.sqrt(total_down)
    narrow_gate, narrow_up, narrow_down = (
        (master_gate / jnp.expand_dims(scale_gate, 1)).astype(jnp.bfloat16),
        (master_up / jnp.expand_dims(scale_up, 1)).astype(jnp.bfloat16),
        (master_down / jnp.expand_dims(scale_down, 2)).astype(jnp.bfloat16),
    )
    final_gate, final_up = (
        lax.all_to_all(narrow_gate, "shard", split_axis=2, concat_axis=1, tiled=True),
        lax.all_to_all(narrow_up, "shard", split_axis=2, concat_axis=1, tiled=True),
    )
    final_down = lax.all_to_all(narrow_down, "shard", split_axis=1, concat_axis=2, tiled=True)
    scale_gate = lax.dynamic_slice_in_dim(
        scale_gate, lax.axis_index("shard") * final_gate.shape[2], final_gate.shape[2], axis=1
    )
    scale_up = lax.dynamic_slice_in_dim(
        scale_up, lax.axis_index("shard") * final_up.shape[2], final_up.shape[2], axis=1
    )
    scale_down = lax.dynamic_slice_in_dim(
        scale_down, lax.axis_index("shard") * final_down.shape[1], final_down.shape[1], axis=1
    )
    part_router = (router_weight * router_gain[:, None]).astype(jnp.bfloat16)
    row_router = lax.all_gather(part_router, "shard", axis=0, tiled=True)
    serve_router = lax.all_gather(row_router, "expert", axis=1, tiled=True)
    return (final_gate, final_up, final_down, scale_gate, scale_up, scale_down, serve_router)


def on_device(n, groups, gate, up, down, router_weight, router_gain):
    experts, rows, width = gate.shape
    cols = width // n
    inner = down.shape[2]
    depth, experts_here = router_weight.shape
    if cols % 128 or inner % 128 or depth % 128:
        return by_collectives(gate, up, down, router_weight, router_gain)
    narrow, wide = jnp.bfloat16, jnp.float32
    early = experts - max(1, experts // 8)
    dma = pltpu.SemaphoreType.DMA
    any_space = pl.BlockSpec(memory_space=pl.ANY)
    vmem = pl.BlockSpec(memory_space=pltpu.VMEM)
    outs = pl.pallas_call(
        functools.partial(exchange, n, groups),
        out_shape=(
            jax.ShapeDtypeStruct((experts, rows * n, cols), narrow),
            jax.ShapeDtypeStruct((experts, rows * n, cols), narrow),
            jax.ShapeDtypeStruct((early, cols, inner * n), narrow),
            jax.ShapeDtypeStruct((experts, cols), wide),
            jax.ShapeDtypeStruct((experts, cols), wide),
            jax.ShapeDtypeStruct((experts, cols), wide),
            jax.ShapeDtypeStruct((experts_here * groups, depth * n), narrow),
            jax.ShapeDtypeStruct((n, experts - early, cols, inner), narrow),
        ),
        in_specs=[any_space] * 3 + [vmem] * 2,
        out_specs=(any_space,) * 3 + (vmem,) * 3 + (any_space,) * 2,
        scratch_shapes=[
            pltpu.VMEM((SLOTS, rows, width), wide),
            pltpu.VMEM((SLOTS, rows, width), wide),
            pltpu.VMEM((SLOTS, width, inner), wide),
            pltpu.VMEM((experts, n, rows, cols), narrow),
            pltpu.VMEM((experts, n, rows, cols), narrow),
            pltpu.VMEM((experts, n, cols, inner), narrow),
            pltpu.VMEM((experts, n, 3, 1, cols), wide),
            pltpu.VMEM((experts, n - 1, 3, 1, cols), wide),
            pltpu.VMEM((experts, 3, 1, cols), wide),
            pltpu.VMEM((experts, n, 3, 1, cols), wide),
            pltpu.VMEM((experts_here, depth), narrow),
            dma((SLOTS, 3)),
            dma,
            dma((experts,)),
            dma,
            dma((experts,)),
            dma((3,)),
            dma((3,)),
            dma((4,)),
            dma((5,)),
        ],
        compiler_params=pltpu.CompilerParams(
            collective_id=0, has_side_effects=True, vmem_limit_bytes=60 * 2**20
        ),
    )(gate, up, down, router_weight.T, router_gain[None, :])
    late = lax.all_to_all(outs[7], "shard", split_axis=0, concat_axis=0, tiled=True)

    def one(shape, cap):
        block = (1,) + shape[1:]
        return pl.BlockSpec(block, lambda t: (jnp.minimum(t, cap - 1), 0, 0))

    specs = [
        one(outs[0].shape, experts),
        one(outs[1].shape, experts),
        one(outs[2].shape, early),
    ] + [pl.BlockSpec(x.shape, lambda t: (0, 0)) for x in outs[3:7]]
    full = jax.ShapeDtypeStruct((experts, cols, inner * n), narrow)
    moved = sum(x.size * x.dtype.itemsize for x in outs[:7])
    placed = pl.pallas_call(
        place,
        grid=(experts,),
        in_specs=specs,
        out_specs=specs,
        out_shape=tuple(
            full if i == 2 else jax.ShapeDtypeStruct(x.shape, x.dtype)
            for i, x in enumerate(outs[:7])
        ),
        compiler_params=pltpu.CompilerParams(dimension_semantics=("arbitrary",)),
        cost_estimate=pl.CostEstimate(flops=0, bytes_accessed=2 * moved, transcendentals=0),
    )(*outs[:7])
    final_down = pl.pallas_call(
        functools.partial(place_late, n, early),
        in_specs=[any_space] * 2,
        out_specs=any_space,
        out_shape=full,
        input_output_aliases={0: 0},
        scratch_shapes=[dma((n,))],
        compiler_params=pltpu.CompilerParams(vmem_limit_bytes=2**20),
    )(placed[2], late)
    return placed[:2] + (final_down,) + placed[3:6] + (placed[6].T,)


def place(*refs):
    half = len(refs) // 2
    for src, dst in zip(refs[:half], refs[half:]):
        dst[...] = src[...]


def place_late(n, early, _, late, out, sem):
    inner = late.shape[3]
    copies = [
        pltpu.make_async_copy(
            late.at[d],
            out.at[pl.ds(early, late.shape[1]), :, pl.ds(d * inner, inner)],
            sem.at[d],
        )
        for d in range(n)
    ]
    for copy in copies:
        copy.start()
    for copy in copies:
        copy.wait()


def solution(mesh):
    placed = (
        P("expert", "shard", None),
        P("expert", "shard", None),
        P("expert", None, "shard"),
        P("shard", "expert"),
        P("shard"),
    )
    return jax.shard_map(
        functools.partial(on_device, mesh.shape["shard"], mesh.shape["expert"]),
        mesh=mesh,
        in_specs=placed,
        out_specs=(
            P("expert", None, "shard"),
            P("expert", None, "shard"),
            P("expert", "shard", None),
            P("expert", "shard"),
            P("expert", "shard"),
            P("expert", "shard"),
            P(),
        ),
        check_vma=False,
    )
```
